512 devices in a mesh: groups: 2 (over y), seq: 16 (over z), head: 8 (over x), rep: 2 (over core).
Axes of the slice: x: 8, y: 2, z: 16, core: 2. Of those that a mesh axis runs over, the one named last changes fastest.
The devices are a block of a 8x8x16 slice.
Arguments:
- q_latent: bfloat16 [32, 2, 128, 512], P('groups', None, 'head'), parts along dimension 0, may hold values from -40 to 40
- q_rope: bfloat16 [32, 2, 128, 64], P('groups', None, 'head'), parts along dimension 0, may hold values from -40 to 40
- cache_latent: bfloat16 [32, 2048, 512], P(('groups', 'rep'), 'seq'), parts along dimension 0, may hold values from -20 to 20
- rope_keys: bfloat16 [32, 64, 2048], P(('groups', 'rep'), None, 'seq'), parts along dimension 0, may hold values from -20 to 20
- lengths: int32 [32], P(('groups', 'rep')), parts along dimension 0, may hold values from 128 to 2048, as said below
- slot_request: int32 [32], P(('groups', 'rep')), parts along dimension 0, may hold values from 0 to 15, as said below
- value_up: bfloat16 [128, 512, 128], P('head'), may hold values from -0.25 to 0.25
Outputs:
- values: bfloat16 [32, 2, 128, 128], P(('groups', 'rep'), None, 'head'), parts along dimension 0
The draws below stay inside these ranges and needn't reach their ends.
There are 2 independent parts, one for each index of `groups`. The reference program is written for one: setup_inputs(seed, part) draws one part's arguments, and reference() takes and returns one part's arrays. A program takes and returns all parts, laid end to end along the dimension named above; an argument that names none is the same for every part. Nothing has to cross between parts.
Inputs may be any that keep to these rules, and one draw needn't show every extreme that they name: `lengths`: each slot's length lies between 128 and 2048; in every part some slot holds 2048. `slot_request`: a permutation of the requests 0 to 15.
All inputs are finite; a program needn't handle non-finite values.
Results may differ from the reference program's by a relative error of at most 0.0021.
Values may be sent and summed in bfloat16 or wider, within the bound.
No kernel may reach another device: no remote copies, remote signals or barrier semaphores. Data moves between devices by JAX's collectives and lax.ppermute only.
A program may use at most 64 MiB of HBM per device.

```python
import jax
import jax.numpy as jnp
from jax import lax

HEADS = 128
LATENT = 512
ROPE = 64
NOPE = 128
DV = 128
QTOK = 2
PAGE = 128
BATCH = 16
SEQ_LEN = 2048


def slot_order(key):
    return jax.random.permutation(jax.random.fold_in(key, 11), BATCH).astype(jnp.int32)


def cache_parts(key):
    latent = jax.random.truncated_normal(jax.random.fold_in(key, 12), -5.0, 5.0, (BATCH, SEQ_LEN, LATENT), jnp.float32)
    rotary = jax.random.truncated_normal(jax.random.fold_in(key, 13), -5.0, 5.0, (BATCH, ROPE, SEQ_LEN), jnp.float32)
    return (latent, rotary)


def shared_queries(key):
    lat_shape = (BATCH, QTOK, HEADS, LATENT)
    rot_shape = (BATCH, QTOK, HEADS, ROPE)
    query_lat = 2.0 * jax.random.truncated_normal(jax.random.fold_in(key, 21), -5.0, 5.0, lat_shape, jnp.float32)
    query_rot = 2.0 * jax.random.truncated_normal(jax.random.fold_in(key, 22), -5.0, 5.0, rot_shape, jnp.float32)
    return (query_lat, query_rot)


def draw_q_latent(key, part):
    return shared_queries(key)[0].astype(jnp.bfloat16)


def draw_q_rope(key, part):
    return shared_queries(key)[1].astype(jnp.bfloat16)


def draw_cache_latent(key, part):
    return cache_parts(key)[0].astype(jnp.bfloat16)


def draw_rope_keys(key, part):
    return cache_parts(key)[1].astype(jnp.bfloat16)


def draw_lengths(key, part):
    drawn = jax.random.randint(jax.random.fold_in(key, 31), (BATCH,), PAGE, SEQ_LEN + 1)
    longest = jax.random.randint(jax.random.fold_in(key, 32), (), 0, BATCH)
    return drawn.at[longest].set(SEQ_LEN).astype(jnp.int32)


def draw_slot_request(key, part):
    return slot_order(key)


def level_of(key, dims, pieces, least, top_value):
    level = 1.0
    for dim, parts in pieces:
        heights = jax.random.uniform(jax.random.fold_in(jax.random.fold_in(key, 6), dim), (parts,), jnp.float32, least / len(pieces), top_value / len(pieces))
        level = level * jnp.repeat(jnp.exp(heights), dims[dim] // parts).reshape((-1,) + (1,) * (len(dims) - 1 - dim))
    return level


def gaussian(rng, shape, width, bound, cuts=(), kind=jnp.bfloat16):
    values = width * jax.random.normal(rng, shape, jnp.float32)
    if cuts:
        values = values * level_of(rng, shape, cuts, -0.22, 0.18)
    return jnp.clip(values, -bound, bound).astype(kind)


def setup_inputs(seed: int = 0, part: int = 0) -> dict:
    streams_of = jax.random.split(jax.random.key(seed), 8)
    part_keys = jax.random.split(jax.random.fold_in(streams_of[7], part), 8)
    return {
        "q_latent": draw_q_latent(jax.random.fold_in(jax.random.fold_in(streams_of[7], part), 71), part),
        "q_rope": draw_q_rope(jax.random.fold_in(jax.random.fold_in(streams_of[7], part), 71), part),
        "cache_latent": draw_cache_latent(jax.random.fold_in(jax.random.fold_in(streams_of[7], part), 71), part),
        "rope_keys": draw_rope_keys(jax.random.fold_in(jax.random.fold_in(streams_of[7], part), 71), part),
        "lengths": draw_lengths(jax.random.fold_in(jax.random.fold_in(streams_of[7], part), 71), part),
        "slot_request": draw_slot_request(jax.random.fold_in(jax.random.fold_in(streams_of[7], part), 71), part),
        "value_up": gaussian(streams_of[6], (HEADS, LATENT, DV), LATENT ** -0.5, 0.25, ((0, 8),)),
    }


negative_fill = -1e30


def reference(q_latent, q_rope, cache_latent, rope_keys, lengths, slot_request, value_up):
    softmax_scale = (NOPE + ROPE) ** -0.5
    page_count = SEQ_LEN // PAGE
    weight = value_up.astype(jnp.float32)

    def per_slot(slot_index):
        request = slot_request[slot_index]
        query_lat = q_latent[request].astype(jnp.float32)
        query_rot = q_rope[request].astype(jnp.float32)
        cache_rows = cache_latent[slot_index].astype(jnp.float32)
        rope_rows = rope_keys[slot_index].astype(jnp.float32)
        scores = jnp.einsum("thd,pd->thp", query_lat, cache_rows)
        scores = (scores + jnp.einsum("the,ep->thp", query_rot, rope_rows)) * softmax_scale
        positions = jnp.arange(SEQ_LEN, dtype=jnp.int32)
        limits = lengths[slot_index] - QTOK + 1 + jnp.arange(QTOK, dtype=jnp.int32)
        visible = positions[None, :] < limits[:, None]
        visible = jnp.broadcast_to(visible[:, None, :], scores.shape).reshape(QTOK, HEADS, page_count, PAGE)
        masked = jnp.where(visible, scores.reshape(QTOK, HEADS, page_count, PAGE), negative_fill)
        page_max = jnp.max(masked, axis=3)
        page_exp = jnp.where(visible, jnp.exp(masked - page_max[..., None]), 0.0)
        page_den = jnp.sum(page_exp, axis=3)
        page_weights = lax.optimization_barrier(page_exp.astype(jnp.bfloat16)).astype(jnp.float32)
        page_out = jnp.einsum("thnp,npd->thnd", page_weights, cache_rows.reshape(page_count, PAGE, LATENT))
        largest = jnp.max(page_max, axis=2)
        factor = jnp.exp(page_max - largest[..., None])
        denominator = jnp.sum(factor * page_den, axis=2)
        summed = jnp.sum(factor[..., None] * page_out, axis=2)
        attended = summed / denominator[..., None]
        result = jnp.einsum("thd,hdv->thv", attended, weight, precision=lax.Precision.HIGHEST)
        return result.astype(jnp.bfloat16)

    return lax.map(per_slot, jnp.arange(BATCH, dtype=jnp.int32))
```

```python
import functools

import jax
import jax.numpy as jnp
from jax import lax
from jax.experimental import pallas as pl
from jax.experimental.pallas import tpu as pltpu
from jax.sharding import PartitionSpec as P


NOPE = 128
NEGATIVE = -1e30
STEPS = 32768.0
LEAST_EXPONENT = -110.0
WEIGHT_CHUNKS = 4


def decoded(message):
    half = message.shape[0] - 8
    log_weight = message[half : half + 1].astype(jnp.float32) * (1.0 / STEPS)
    exponent = message[half + 1 : half + 2].astype(jnp.float32)
    kept = message[half + 2 : half + 3] > 0
    packed = message[:half]
    high = jnp.right_shift(packed, 16).astype(jnp.float32)
    low = (jnp.bitwise_and(packed, 0xFFFF) - 32768).astype(jnp.float32)
    unit = jnp.exp2(exponent) * (1.0 / STEPS)
    return high, low, unit, log_weight, kept


def encoded(high, low, log_weight, kept):
    top = jnp.maximum(
        jnp.max(jnp.abs(high), axis=0, keepdims=True), jnp.max(jnp.abs(low), axis=0, keepdims=True)
    )
    exponent = jnp.maximum(jnp.ceil(jnp.log2(top)), LEAST_EXPONENT)
    factor = jnp.exp2(-exponent) * STEPS

    def fixed(x):
        return jnp.clip(jnp.round(x * factor), -32767.0, 32767.0).astype(jnp.int32)

    packed = fixed(high) * 65536 + (fixed(low) + 32768)
    rows = packed.shape[1]
    at = lax.broadcasted_iota(jnp.int32, (8, rows), 0)
    log_fixed = jnp.where(kept, jnp.round(log_weight * STEPS), 0.0).astype(jnp.int32)
    side = jnp.where(at == 0, log_fixed, 0)
    side = jnp.where(at == 1, exponent.astype(jnp.int32), side)
    side = jnp.where(at == 2, kept.astype(jnp.int32), side)
    return packed, side


def merged(messages):
    parts = [decoded(m) for m in messages]
    largest = functools.reduce(jnp.maximum, [jnp.where(p[4], p[3], NEGATIVE) for p in parts])
    weights = [jnp.where(p[4], jnp.exp(p[3] - largest), 0.0) for p in parts]
    total = sum(weights)
    kept = total > 0.0
    inverse = 1.0 / jnp.where(kept, total, 1.0)
    scales = [w * inverse * p[2] for w, p in zip(weights, parts)]
    high = sum(s * p[0] for s, p in zip(scales, parts))
    low = sum(s * p[1] for s, p in zip(scales, parts))
    return high, low, largest + jnp.log(jnp.where(kept, total, 1.0)), kept


def partial_kernel(
    lengths, slots, q_lat_hbm, q_rot_hbm, cache_hbm, rope_hbm, up_hbm, out_ref,
    q_lat, q_rot, cache, rope, up, attended, values, side, sems, cache_sems, rope_sems, up_sems,
):
    n_slots, page_len, latent = cache.shape
    _, tokens, heads, _ = q_lat.shape
    rows = tokens * heads
    step = heads // WEIGHT_CHUNKS
    copy = pltpu.make_async_copy
    q_copies = [copy(q_lat_hbm, q_lat, sems.at[0]), copy(q_rot_hbm, q_rot, sems.at[1])]
    cache_copies = [copy(cache_hbm.at[b], cache.at[b], cache_sems.at[b]) for b in range(n_slots)]
    rope_copies = [copy(rope_hbm.at[b], rope.at[b], rope_sems.at[b]) for b in range(n_slots)]
    up_copies = [
        copy(up_hbm.at[pl.ds(i * step, step)], up.at[pl.ds(i * step, step)], up_sems.at[i])
        for i in range(WEIGHT_CHUNKS)
    ]
    for c in q_copies:
        c.start()
    for pair in zip(cache_copies, rope_copies):
        for c in pair:
            c.start()
    for c in up_copies:
        c.start()
    softmax_scale = (NOPE + q_rot.shape[3]) ** -0.5
    first = lax.axis_index("seq") * page_len
    position = first + lax.broadcasted_iota(jnp.int32, (rows, page_len), 1)
    token = (lax.broadcasted_iota(jnp.int32, (rows, page_len), 0) >= heads).astype(jnp.int32)
    lane = lax.broadcasted_iota(jnp.int32, (rows, 128), 1)
    for c in q_copies:
        c.wait()
    for b in range(n_slots):
        request = slots[b]
        cache_copies[b].wait()
        rope_copies[b].wait()
        q1 = q_lat[request].reshape(rows, latent)
        q2 = q_rot[request].reshape(rows, -1)
        keys = cache[b]
        scores = lax.dot_general(
            q1, keys, (((1,), (1,)), ((), ())), preferred_element_type=jnp.float32
        )
        scores += jnp.dot(q2, rope[b], preferred_element_type=jnp.float32)
        visible = position < lengths[b] - (tokens - 1) + token
        masked = jnp.where(visible, scores * softmax_scale, NEGATIVE)
        page_max = jnp.max(masked, axis=1, keepdims=True)
        page_exp = jnp.where(visible, jnp.exp(masked - page_max), 0.0)
        page_den = jnp.sum(page_exp, axis=1, keepdims=True)
        kept = page_den > 0.0
        safe = jnp.where(kept, page_den, 1.0)
        page_out = jnp.dot(
            page_exp.astype(jnp.bfloat16), keys, preferred_element_type=jnp.float32
        )
        page_out *= 1.0 / safe
        for j in range(latent // 128):
            attended[j, pl.ds(b * rows, rows), :] = page_out[:, j * 128 : (j + 1) * 128]
        log_weight = page_max + jnp.log(safe)
        side[pl.ds(b * rows, rows), :] = jnp.where(
            lane == 0, log_weight, jnp.where(lane == 1, kept.astype(jnp.float32), 0.0)
        )
    pairs = n_slots * tokens
    for h in range(heads):
        if h % step == 0:
            up_copies[h // step].wait()
        x = jnp.concatenate(
            [attended[j, pl.ds(h, pairs, stride=heads), :] for j in range(latent // 128)], axis=1
        )
        high = x.astype(jnp.bfloat16)
        low = (x - high.astype(jnp.float32)).astype(jnp.bfloat16)
        y = jnp.dot(
            jnp.concatenate([high, low], axis=0), up[h], preferred_element_type=jnp.float32
        )
        values[pl.ds(h, pairs, stride=heads), :] = y[:pairs] + y[pairs:]
    columns = values[...].T
    sides = side[...].T
    half = columns.shape[0] // 2
    packed, words = encoded(columns[:half], columns[half:], sides[0:1], sides[1:2] > 0.5)
    out_ref[pl.ds(0, half), :] = packed
    out_ref[pl.ds(half, 8), :] = words


def local_message(q_latent, q_rope, cache_latent, rope_keys, lengths, slot_request, value_up):
    n_slots, _, latent = cache_latent.shape
    _, tokens, heads, _ = q_rope.shape
    dv = value_up.shape[2]
    rows = n_slots * tokens * heads
    hbm = pl.BlockSpec(memory_space=pl.ANY)
    smem = pl.BlockSpec(memory_space=pltpu.SMEM)
    return pl.pallas_call(
        partial_kernel,
        name="local_message",
        out_shape=pltpu.VMEM((dv // 2 + 8, rows), jnp.int32),
        in_specs=[smem, smem, hbm, hbm, hbm, hbm, hbm],
        out_specs=pl.BlockSpec(memory_space=pltpu.VMEM),
        scratch_shapes=[
            pltpu.VMEM(q_latent.shape, q_latent.dtype),
            pltpu.VMEM(q_rope.shape, q_rope.dtype),
            pltpu.VMEM(cache_latent.shape, cache_latent.dtype),
            pltpu.VMEM(rope_keys.shape, rope_keys.dtype),
            pltpu.VMEM(value_up.shape, value_up.dtype),
            pltpu.VMEM((latent // 128, rows, 128), jnp.float32),
            pltpu.VMEM((rows, dv), jnp.float32),
            pltpu.VMEM((rows, 128), jnp.float32),
            pltpu.SemaphoreType.DMA((2,)),
            pltpu.SemaphoreType.DMA((n_slots,)),
            pltpu.SemaphoreType.DMA((n_slots,)),
            pltpu.SemaphoreType.DMA((WEIGHT_CHUNKS,)),
        ],
    )(lengths, slot_request, q_latent, q_rope, cache_latent, rope_keys, value_up)


def merge_kernel(*refs):
    *ins, out_ref = refs
    half = out_ref.shape[0] - 8
    packed, words = encoded(*merged([r[...] for r in ins]))
    out_ref[pl.ds(0, half), :] = packed
    out_ref[pl.ds(half, 8), :] = words


def merge(*messages):
    vmem = pl.BlockSpec(memory_space=pltpu.VMEM)
    return pl.pallas_call(
        merge_kernel,
        name="merge",
        out_shape=pltpu.VMEM(messages[0].shape, jnp.int32),
        in_specs=[vmem] * len(messages),
        out_specs=vmem,
    )(*[pltpu.with_memory_space_constraint(m, pltpu.VMEM) for m in messages])


def finish_kernel(root, *refs):
    *ins, out_ref = refs
    high, low, _, _ = merged([r[...] for r in ins])
    whole = jnp.concatenate([high, low], axis=0)
    mine = lax.axis_index("seq") == root
    out_ref[...] = jnp.where(mine, whole.T, 0.0).astype(out_ref.dtype)


def finish(root, messages):
    half, rows = messages[0].shape
    vmem = pl.BlockSpec(memory_space=pltpu.VMEM)
    return pl.pallas_call(
        functools.partial(finish_kernel, root),
        name="finish",
        out_shape=pltpu.VMEM((rows, 2 * (half - 8)), jnp.bfloat16),
        in_specs=[vmem] * len(messages),
        out_specs=vmem,
    )(*[pltpu.with_memory_space_constraint(m, pltpu.VMEM) for m in messages])


def send(x, *pairs):
    return lax.ppermute(x, "seq", pairs)


ROOT = 1
LATE = (15, 10, 11, 12, 13, 14, 0, 9, 8)
EARLY = (7, 6, 5, 4, 3, 2)
RELAY = 15
TOLD = (0, 2, RELAY)
RELAYED = (3, 4, 5, 6, 7)
SPREAD = (((7, 8), (6, 9), (5, 10), (15, 14)), ((7, 11), (6, 12), (15, 13)))


def per_device(q_latent, q_rope, cache_latent, rope_keys, lengths, slot_request, value_up):
    own = local_message(q_latent, q_rope, cache_latent, rope_keys, lengths, slot_request, value_up)
    arrived = {z: send(own, (z, ROOT)) for z in LATE + EARLY}
    near = merge(own, *[arrived[z] for z in EARLY])
    held = finish(ROOT, [near, *[arrived[z] for z in LATE]])
    told = {z: send(held, (ROOT, z)) for z in TOLD}
    held = held + told.pop(RELAY)
    relayed = [send(held, (RELAY, z)) for z in RELAYED]
    held = sum(relayed, held)
    spread = [send(held, *pairs) for pairs in SPREAD]
    held = sum([*spread, *told.values()], held)
    n_slots, (_, tokens, heads, _) = cache_latent.shape[0], q_rope.shape
    return held.reshape(n_slots, tokens, heads, -1)


def solution(mesh):
    in_specs = (
        P("groups", None, "head", None),
        P("groups", None, "head", None),
        P(("groups", "rep"), "seq", None),
        P(("groups", "rep"), None, "seq"),
        P(("groups", "rep")),
        P(("groups", "rep")),
        P("head", None, None),
    )
    out_specs = P(("groups", "rep"), None, "head", None)
    return jax.shard_map(
        per_device, mesh=mesh, in_specs=in_specs, out_specs=out_specs, check_vma=False
    )
```

```python
import functools

import jax
import jax.numpy as jnp
from jax import lax
from jax.experimental import pallas as pl
from jax.experimental.pallas import tpu as pltpu
from jax.sharding import PartitionSpec as P


NOPE = 128
NEGATIVE = -1e30
STEPS = 32768.0
LEAST_EXPONENT = -110.0
WEIGHT_CHUNKS = 1
PAGE_GROUPS = 1


def decoded(message):
    half = message.shape[0] - 8
    log_weight = message[half : half + 1].astype(jnp.float32) * (1.0 / STEPS)
    exponent = message[half + 1 : half + 2].astype(jnp.float32)
    kept = message[half + 2 : half + 3] > 0
    packed = message[:half]
    high = jnp.right_shift(packed, 16).astype(jnp.float32)
    low = (jnp.bitwise_and(packed, 0xFFFF) - 32768).astype(jnp.float32)
    unit = jnp.exp2(exponent) * (1.0 / STEPS)
    return high, low, unit, log_weight, kept


def encoded(high, low, log_weight, kept):
    top = jnp.maximum(
        jnp.max(jnp.abs(high), axis=0, keepdims=True), jnp.max(jnp.abs(low), axis=0, keepdims=True)
    )
    exponent = jnp.maximum(jnp.ceil(jnp.log2(top)), LEAST_EXPONENT)
    factor = jnp.exp2(-exponent) * STEPS

    def fixed(x):
        return jnp.clip(jnp.round(x * factor), -32767.0, 32767.0).astype(jnp.int32)

    packed = fixed(high) * 65536 + (fixed(low) + 32768)
    rows = packed.shape[1]
    at = lax.broadcasted_iota(jnp.int32, (8, rows), 0)
    log_fixed = jnp.where(kept, jnp.round(log_weight * STEPS), 0.0).astype(jnp.int32)
    side = jnp.where(at == 0, log_fixed, 0)
    side = jnp.where(at == 1, exponent.astype(jnp.int32), side)
    side = jnp.where(at == 2, kept.astype(jnp.int32), side)
    return packed, side


def merged(messages):
    parts = [decoded(m) for m in messages]
    largest = functools.reduce(jnp.maximum, [jnp.where(p[4], p[3], NEGATIVE) for p in parts])
    weights = [jnp.where(p[4], jnp.exp(p[3] - largest), 0.0) for p in parts]
    total = sum(weights)
    kept = total > 0.0
    inverse = 1.0 / jnp.where(kept, total, 1.0)
    scales = [w * inverse * p[2] for w, p in zip(weights, parts)]
    high = sum(s * p[0] for s, p in zip(scales, parts))
    low = sum(s * p[1] for s, p in zip(scales, parts))
    return high, low, largest + jnp.log(jnp.where(kept, total, 1.0)), kept


def partial_kernel(
    lengths_hbm, slots_hbm, q_lat_hbm, q_rot_hbm, cache_hbm, rope_hbm, up_hbm, out_ref,
    lengths, slots, q_lat, q_rot, cache, rope, up, attended, values, side, sems, page_sems, up_sems,
):
    n_slots, page_len, latent = cache.shape
    _, tokens, heads, _ = q_lat.shape
    rows = tokens * heads
    step = heads // WEIGHT_CHUNKS
    group = n_slots // PAGE_GROUPS
    copy = pltpu.make_async_copy
    scalars = [copy(lengths_hbm, lengths, sems.at[0]), copy(slots_hbm, slots, sems.at[1])]
    queries = [copy(q_lat_hbm, q_lat, sems.at[2]), copy(q_rot_hbm, q_rot, sems.at[3])]
    pages = []
    for g in range(PAGE_GROUPS):
        at = pl.ds(g * group, group)
        pages.append(
            [
                copy(cache_hbm.at[at], cache.at[at], page_sems.at[g, 0]),
                copy(rope_hbm.at[at], rope.at[at], page_sems.at[g, 1]),
            ]
        )
    ups = [
        copy(up_hbm.at[pl.ds(i * step, step)], up.at[pl.ds(i * step, step)], up_sems.at[i])
        for i in range(WEIGHT_CHUNKS)
    ]
    for c in [*scalars, *queries, *sum(pages, []), *ups]:
        c.start()
    softmax_scale = (NOPE + q_rot.shape[3]) ** -0.5
    first = lax.axis_index("seq") * page_len
    token = (lax.broadcasted_iota(jnp.int32, (rows, page_len), 0) >= heads).astype(jnp.int32)
    offset = first + lax.broadcasted_iota(jnp.int32, (rows, page_len), 1) - token + (tokens - 1)
    lane = lax.broadcasted_iota(jnp.int32, (rows, 128), 1)
    for c in [*scalars, *queries]:
        c.wait()
    for g in range(PAGE_GROUPS):
        for c in pages[g]:
            c.wait()
        members = range(g * group, (g + 1) * group)
        scores = []
        for b in members:
            request = slots[b]
            q1 = q_lat[request].reshape(rows, latent)
            q2 = q_rot[request].reshape(rows, -1)
            s = lax.dot_general(
                q1, cache[b], (((1,), (1,)), ((), ())), preferred_element_type=jnp.float32
            )
            scores.append(s + jnp.dot(q2, rope[b], preferred_element_type=jnp.float32))
        weights = []
        for b, s in zip(members, scores):
            visible = offset < lengths[b]
            masked = jnp.where(visible, s * softmax_scale, NEGATIVE)
            page_max = jnp.max(masked, axis=1, keepdims=True)
            page_exp = jnp.where(visible, jnp.exp(masked - page_max), 0.0)
            weights.append((page_max, page_exp))
        for b, (page_max, page_exp) in zip(members, weights):
            page_out = jnp.dot(
                page_exp.astype(jnp.bfloat16), cache[b], preferred_element_type=jnp.float32
            )
            page_den = jnp.sum(page_exp, axis=1, keepdims=True)
            kept = page_den > 0.0
            safe = jnp.where(kept, page_den, 1.0)
            page_out *= 1.0 / safe
            for j in range(latent // 128):
                attended[j, pl.ds(b * rows, rows), :] = page_out[:, j * 128 : (j + 1) * 128]
            side[pl.ds(b * rows, rows), :] = jnp.where(
                lane == 0,
                page_max + jnp.log(safe),
                jnp.where(lane == 1, kept.astype(jnp.float32), 0.0),
            )
    pairs = n_slots * tokens
    for h in range(heads):
        if h % step == 0:
            ups[h // step].wait()
        x = jnp.concatenate(
            [attended[j, pl.ds(h, pairs, stride=heads), :] for j in range(latent // 128)], axis=1
        )
        high = x.astype(jnp.bfloat16)
        low = (x - high.astype(jnp.float32)).astype(jnp.bfloat16)
        y = jnp.dot(
            jnp.concatenate([high, low], axis=0), up[h], preferred_element_type=jnp.float32
        )
        values[pl.ds(h, pairs, stride=heads), :] = y[:pairs] + y[pairs:]
    columns = values[...].T
    sides = side[...].T
    half = columns.shape[0] // 2
    packed, words = encoded(columns[:half], columns[half:], sides[0:1], sides[1:2] > 0.5)
    out_ref[pl.ds(0, half), :] = packed
    out_ref[pl.ds(half, 8), :] = words


def local_message(q_latent, q_rope, cache_latent, rope_keys, lengths, slot_request, value_up):
    n_slots = cache_latent.shape[0]
    latent = cache_latent.shape[2]
    _, tokens, heads, _ = q_rope.shape
    dv = value_up.shape[2]
    rows = n_slots * tokens * heads
    return pl.pallas_call(
        partial_kernel,
        name="local_message",
        out_shape=pltpu.VMEM((dv // 2 + 8, rows), jnp.int32),
        in_specs=[pl.BlockSpec(memory_space=pl.ANY)] * 7,
        out_specs=pl.BlockSpec(memory_space=pltpu.VMEM),
        scratch_shapes=[
            pltpu.SMEM(lengths.shape, jnp.int32),
            pltpu.SMEM(slot_request.shape, jnp.int32),
            pltpu.VMEM(q_latent.shape, q_latent.dtype),
            pltpu.VMEM(q_rope.shape, q_rope.dtype),
            pltpu.VMEM(cache_latent.shape, cache_latent.dtype),
            pltpu.VMEM(rope_keys.shape, rope_keys.dtype),
            pltpu.VMEM(value_up.shape, value_up.dtype),
            pltpu.VMEM((latent // 128, rows, 128), jnp.float32),
            pltpu.VMEM((rows, dv), jnp.float32),
            pltpu.VMEM((rows, 128), jnp.float32),
            pltpu.SemaphoreType.DMA((4,)),
            pltpu.SemaphoreType.DMA((PAGE_GROUPS, 2)),
            pltpu.SemaphoreType.DMA((WEIGHT_CHUNKS,)),
        ],
    )(lengths, slot_request, q_latent, q_rope, cache_latent, rope_keys, value_up)


def merge_kernel(*refs):
    *ins, out_ref = refs
    half = out_ref.shape[0] - 8
    packed, words = encoded(*merged([r[...] for r in ins]))
    out_ref[pl.ds(0, half), :] = packed
    out_ref[pl.ds(half, 8), :] = words


def merge(*messages):
    vmem = pl.BlockSpec(memory_space=pltpu.VMEM)
    return pl.pallas_call(
        merge_kernel,
        name="merge",
        out_shape=pltpu.VMEM(messages[0].shape, jnp.int32),
        in_specs=[vmem] * len(messages),
        out_specs=vmem,
    )(*[pltpu.with_memory_space_constraint(m, pltpu.VMEM) for m in messages])


def finish_kernel(root, *refs):
    *ins, out_ref = refs
    high, low, _, _ = merged([r[...] for r in ins])
    whole = jnp.concatenate([high, low], axis=0)
    mine = lax.axis_index("seq") == root
    out_ref[...] = jnp.where(mine, whole.T, 0.0).astype(out_ref.dtype)


def finish(root, messages):
    half, rows = messages[0].shape
    vmem = pl.BlockSpec(memory_space=pltpu.VMEM)
    return pl.pallas_call(
        functools.partial(finish_kernel, root),
        name="finish",
        out_shape=pltpu.VMEM((rows, 2 * (half - 8)), jnp.bfloat16),
        in_specs=[vmem] * len(messages),
        out_specs=vmem,
    )(*[pltpu.with_memory_space_constraint(m, pltpu.VMEM) for m in messages])


def send(x, *pairs):
    return lax.ppermute(x, "seq", pairs)


ROOT = 2
LATE = (15, 10, 11, 12, 13, 14, 0, 9, 8)
TREE = (((3, 2), (7, 6), (5, 4)), ((1, 2), (6, 4)), ((4, 2),))
FAN = (
    ('fan0', (), ((2, 0),)),
    ('fan1', (), ((2, 5),)),
    ('fan2', (), ((2, 1),)),
    ('fan3', ('fan1',), ((5, 3),)),
    ('fan4', ('fan1',), ((5, 4),)),
    ('fan5', ('fan1',), ((5, 8),)),
    ('fan6', ('fan1',), ((5, 12),)),
    ('fan7', ('fan1', 'fan5', 'fan6'), ((5, 6), (8, 10), (12, 14))),
    ('fan8', ('fan1', 'fan5', 'fan6', 'fan7'), ((5, 7), (8, 9), (10, 11), (12, 13), (14, 15))),
)


def per_device(q_latent, q_rope, cache_latent, rope_keys, lengths, slot_request, value_up):
    own = local_message(q_latent, q_rope, cache_latent, rope_keys, lengths, slot_request, value_up)
    late = [send(own, (z, ROOT)) for z in LATE]
    near = [own]
    for i, pairs in enumerate(TREE):
        if i:
            near = [merge(*near)]
        near.append(send(near[0], *pairs))
    held = finish(ROOT, [*near, *late])
    got = {}
    for name, needs, pairs in FAN:
        got[name] = send(sum([got[n] for n in needs], held), *pairs)
    held = sum(got.values(), held)
    n_slots, (_, tokens, heads, _) = cache_latent.shape[0], q_rope.shape
    return held.reshape(n_slots, tokens, heads, -1)


def solution(mesh):
    in_specs = (
        P("groups", None, "head", None),
        P("groups", None, "head", None),
        P(("groups", "rep"), "seq", None),
        P(("groups", "rep"), None, "seq"),
        P(("groups", "rep")),
        P(("groups", "rep")),
        P("head", None, None),
    )
    out_specs = P(("groups", "rep"), None, "head", None)
    return jax.shard_map(
        per_device, mesh=mesh, in_specs=in_specs, out_specs=out_specs, check_vma=False
    )
```

```python
import functools

import jax
import jax.numpy as jnp
from jax import lax
from jax.experimental import pallas as pl
from jax.experimental.pallas import tpu as pltpu
from jax.sharding import PartitionSpec as P


NOPE = 128
NEGATIVE = -1e30
STEPS = 32768.0
LEAST_EXPONENT = -110.0
WEIGHT_CHUNKS = 1
PAGE_GROUPS = 1


def decoded(message):
    half = message.shape[0] - 8
    log_weight = message[half : half + 1].astype(jnp.float32) * (1.0 / STEPS)
    exponent = message[half + 1 : half + 2].astype(jnp.float32)
    kept = message[half + 2 : half + 3] > 0
    packed = message[:half]
    high = jnp.right_shift(packed, 16).astype(jnp.float32)
    low = (jnp.bitwise_and(packed, 0xFFFF) - 32768).astype(jnp.float32)
    unit = jnp.exp2(exponent) * (1.0 / STEPS)
    return high, low, unit, log_weight, kept


def encoded(high, low, log_weight, kept):
    top = jnp.maximum(
        jnp.max(jnp.abs(high), axis=0, keepdims=True), jnp.max(jnp.abs(low), axis=0, keepdims=True)
    )
    exponent = jnp.maximum(jnp.ceil(jnp.log2(top)), LEAST_EXPONENT)
    factor = jnp.exp2(-exponent) * STEPS

    def fixed(x):
        return jnp.clip(jnp.round(x * factor), -32767.0, 32767.0).astype(jnp.int32)

    packed = fixed(high) * 65536 + (fixed(low) + 32768)
    rows = packed.shape[1]
    at = lax.broadcasted_iota(jnp.int32, (8, rows), 0)
    log_fixed = jnp.where(kept, jnp.round(log_weight * STEPS), 0.0).astype(jnp.int32)
    side = jnp.where(at == 0, log_fixed, 0)
    side = jnp.where(at == 1, exponent.astype(jnp.int32), side)
    side = jnp.where(at == 2, kept.astype(jnp.int32), side)
    return packed, side


def merged(messages):
    parts = [decoded(m) for m in messages]
    largest = functools.reduce(jnp.maximum, [jnp.where(p[4], p[3], NEGATIVE) for p in parts])
    weights = [jnp.where(p[4], jnp.exp(p[3] - largest), 0.0) for p in parts]
    total = sum(weights)
    kept = total > 0.0
    inverse = 1.0 / jnp.where(kept, total, 1.0)
    scales = [w * inverse * p[2] for w, p in zip(weights, parts)]
    high = sum(s * p[0] for s, p in zip(scales, parts))
    low = sum(s * p[1] for s, p in zip(scales, parts))
    return high, low, largest + jnp.log(jnp.where(kept, total, 1.0)), kept


def partial_kernel(
    lengths_hbm, slots_hbm, q_lat_hbm, q_rot_hbm, cache_hbm, rope_hbm, up_hbm, out_ref,
    lengths, slots, q_lat, q_rot, cache, rope, up, attended, values, side, sems, page_sems, up_sems,
):
    n_slots, page_len, latent = cache.shape
    _, tokens, heads, _ = q_lat.shape
    rows = tokens * heads
    step = heads // WEIGHT_CHUNKS
    group = n_slots // PAGE_GROUPS
    copy = pltpu.make_async_copy
    scalars = [copy(lengths_hbm, lengths, sems.at[0]), copy(slots_hbm, slots, sems.at[1])]
    queries = [copy(q_lat_hbm, q_lat, sems.at[2]), copy(q_rot_hbm, q_rot, sems.at[3])]
    pages = []
    for g in range(PAGE_GROUPS):
        at = pl.ds(g * group, group)
        pages.append(
            [
                copy(cache_hbm.at[at], cache.at[at], page_sems.at[g, 0]),
                copy(rope_hbm.at[at], rope.at[at], page_sems.at[g, 1]),
            ]
        )
    ups = [
        copy(up_hbm.at[pl.ds(i * step, step)], up.at[pl.ds(i * step, step)], up_sems.at[i])
        for i in range(WEIGHT_CHUNKS)
    ]
    for c in [*scalars, *queries, *sum(pages, []), *ups]:
        c.start()
    softmax_scale = (NOPE + q_rot.shape[3]) ** -0.5
    first = lax.axis_index("seq") * page_len
    token = (lax.broadcasted_iota(jnp.int32, (rows, page_len), 0) >= heads).astype(jnp.int32)
    offset = first + lax.broadcasted_iota(jnp.int32, (rows, page_len), 1) - token + (tokens - 1)
    lane = lax.broadcasted_iota(jnp.int32, (rows, 128), 1)
    for c in [*scalars, *queries]:
        c.wait()
    for g in range(PAGE_GROUPS):
        for c in pages[g]:
            c.wait()
        members = range(g * group, (g + 1) * group)
        scores = []
        for b in members:
            request = slots[b]
            q1 = q_lat[request].reshape(rows, latent)
            q2 = q_rot[request].reshape(rows, -1)
            s = lax.dot_general(
                q1, cache[b], (((1,), (1,)), ((), ())), preferred_element_type=jnp.float32
            )
            scores.append(s + jnp.dot(q2, rope[b], preferred_element_type=jnp.float32))
        weights = []
        for b, s in zip(members, scores):
            visible = offset < lengths[b]
            masked = jnp.where(visible, s * softmax_scale, NEGATIVE)
            page_max = jnp.max(masked, axis=1, keepdims=True)
            page_exp = jnp.where(visible, jnp.exp(masked - page_max), 0.0)
            weights.append((page_max, page_exp))
        for b, (page_max, page_exp) in zip(members, weights):
            page_out = jnp.dot(
                page_exp.astype(jnp.bfloat16), cache[b], preferred_element_type=jnp.float32
            )
            page_den = jnp.sum(page_exp, axis=1, keepdims=True)
            kept = page_den > 0.0
            safe = jnp.where(kept, page_den, 1.0)
            page_out *= 1.0 / safe
            for j in range(latent // 128):
                attended[j, pl.ds(b * rows, rows), :] = page_out[:, j * 128 : (j + 1) * 128]
            side[pl.ds(b * rows, rows), :] = jnp.where(
                lane == 0,
                page_max + jnp.log(safe),
                jnp.where(lane == 1, kept.astype(jnp.float32), 0.0),
            )
    pairs = n_slots * tokens
    for h in range(heads):
        if h % step == 0:
            ups[h // step].wait()
        x = jnp.concatenate(
            [attended[j, pl.ds(h, pairs, stride=heads), :] for j in range(latent // 128)], axis=1
        )
        high = x.astype(jnp.bfloat16)
        low = (x - high.astype(jnp.float32)).astype(jnp.bfloat16)
        y = jnp.dot(
            jnp.concatenate([high, low], axis=0), up[h], preferred_element_type=jnp.float32
        )
        values[pl.ds(h, pairs, stride=heads), :] = y[:pairs] + y[pairs:]
    columns = values[...].T
    sides = side[...].T
    half = columns.shape[0] // 2
    packed, words = encoded(columns[:half], columns[half:], sides[0:1], sides[1:2] > 0.5)
    out_ref[pl.ds(0, half), :] = packed
    out_ref[pl.ds(half, 8), :] = words


def local_message(q_latent, q_rope, cache_latent, rope_keys, lengths, slot_request, value_up):
    n_slots = cache_latent.shape[0]
    latent = cache_latent.shape[2]
    _, tokens, heads, _ = q_rope.shape
    dv = value_up.shape[2]
    rows = n_slots * tokens * heads
    return pl.pallas_call(
        partial_kernel,
        name="local_message",
        out_shape=pltpu.VMEM((dv // 2 + 8, rows), jnp.int32),
        in_specs=[pl.BlockSpec(memory_space=pl.ANY)] * 7,
        out_specs=pl.BlockSpec(memory_space=pltpu.VMEM),
        scratch_shapes=[
            pltpu.SMEM(lengths.shape, jnp.int32),
            pltpu.SMEM(slot_request.shape, jnp.int32),
            pltpu.VMEM(q_latent.shape, q_latent.dtype),
            pltpu.VMEM(q_rope.shape, q_rope.dtype),
            pltpu.VMEM(cache_latent.shape, cache_latent.dtype),
            pltpu.VMEM(rope_keys.shape, rope_keys.dtype),
            pltpu.VMEM(value_up.shape, value_up.dtype),
            pltpu.VMEM((latent // 128, rows, 128), jnp.float32),
            pltpu.VMEM((rows, dv), jnp.float32),
            pltpu.VMEM((rows, 128), jnp.float32),
            pltpu.SemaphoreType.DMA((4,)),
            pltpu.SemaphoreType.DMA((PAGE_GROUPS, 2)),
            pltpu.SemaphoreType.DMA((WEIGHT_CHUNKS,)),
        ],
    )(lengths, slot_request, q_latent, q_rope, cache_latent, rope_keys, value_up)


def merge_kernel(*refs):
    *ins, out_ref = refs
    half = out_ref.shape[0] - 8
    packed, words = encoded(*merged([r[...] for r in ins]))
    out_ref[pl.ds(0, half), :] = packed
    out_ref[pl.ds(half, 8), :] = words


def merge(*messages):
    vmem = pl.BlockSpec(memory_space=pltpu.VMEM)
    return pl.pallas_call(
        merge_kernel,
        name="merge",
        out_shape=pltpu.VMEM(messages[0].shape, jnp.int32),
        in_specs=[vmem] * len(messages),
        out_specs=vmem,
    )(*[pltpu.with_memory_space_constraint(m, pltpu.VMEM) for m in messages])


def finish_kernel(root, *refs):
    *ins, out_ref = refs
    high, low, _, _ = merged([r[...] for r in ins])
    whole = jnp.concatenate([high, low], axis=0)
    mine = lax.axis_index("seq") == root
    out_ref[...] = jnp.where(mine, whole.T, 0.0).astype(out_ref.dtype)


def finish(root, messages):
    half, rows = messages[0].shape
    vmem = pl.BlockSpec(memory_space=pltpu.VMEM)
    return pl.pallas_call(
        functools.partial(finish_kernel, root),
        name="finish",
        out_shape=pltpu.VMEM((rows, 2 * (half - 8)), jnp.bfloat16),
        in_specs=[vmem] * len(messages),
        out_specs=vmem,
    )(*[pltpu.with_memory_space_constraint(m, pltpu.VMEM) for m in messages])


def send(x, *pairs):
    return lax.ppermute(x, "seq", pairs)


ROOT = 2
GATHER = (
    ('in15', 0, ((15, 2),)),
    ('in10', 0, ((10, 2),)),
    ('in11', 0, ((11, 2),)),
    ('in12', 0, ((12, 2),)),
    ('in13', 0, ((13, 2),)),
    ('in14', 0, ((14, 2),)),
    ('in0', 0, ((0, 2),)),
    ('tree0', 0, ((3, 2), (7, 6), (5, 4), (9, 8))),
    ('in8', 1, ((8, 2),)),
    ('tree1', 1, ((1, 2), (6, 4))),
    ('tree2', 2, ((4, 2),)),
)
FAN = (
    ('fan0', (), ((2, 0),)),
    ('fan1', (), ((2, 1),)),
    ('fan2', (), ((2, 3),)),
    ('fan3', (), ((2, 5),)),
    ('fan4', ('fan3',), ((5, 4),)),
    ('fan5', ('fan3',), ((5, 8),)),
    ('fan6', ('fan3',), ((5, 12),)),
    ('fan7', ('fan3', 'fan5', 'fan6'), ((5, 6), (8, 10), (12, 14))),
    ('fan8', ('fan3', 'fan5', 'fan6', 'fan7'), ((6, 7), (8, 9), (10, 11), (12, 13), (14, 15))),
)


def per_device(q_latent, q_rope, cache_latent, rope_keys, lengths, slot_request, value_up):
    mine = local_message(q_latent, q_rope, cache_latent, rope_keys, lengths, slot_request, value_up)
    level, branches, direct = 0, [], []
    for name, merges, pairs in GATHER:
        if merges > level:
            mine, branches, level = merge(mine, *branches), [], merges
        came = send(mine, *pairs)
        (branches if name.startswith("tree") else direct).append(came)
    held = finish(ROOT, [mine, *branches, *direct])
    got = {}
    for name, needs, pairs in FAN:
        got[name] = send(sum([got[n] for n in needs], held), *pairs)
    held = sum(got.values(), held)
    n_slots, (_, tokens, heads, _) = cache_latent.shape[0], q_rope.shape
    return held.reshape(n_slots, tokens, heads, -1)


def solution(mesh):
    in_specs = (
        P("groups", None, "head", None),
        P("groups", None, "head", None),
        P(("groups", "rep"), "seq", None),
        P(("groups", "rep"), None, "seq"),
        P(("groups", "rep")),
        P(("groups", "rep")),
        P("head", None, None),
    )
    out_specs = P(("groups", "rep"), None, "head", None)
    return jax.shard_map(
        per_device, mesh=mesh, in_specs=in_specs, out_specs=out_specs, check_vma=False
    )
```
